32 devices in a mesh: seq: 4 (over y, core), tp: 8 (over z, x).
Axes of the slice: x: 2, y: 2, z: 4, core: 2. Of those that a mesh axis runs over, the one named last changes fastest.
Arguments:
- tokens: bfloat16 [4096, 5376], P('seq'), may hold values from -6 to 6
- pre_gain: float32 [5376], replicated, may hold values from 0.5 to 2
- w_query: bfloat16 [5376, 4096], P(None, 'tp'), may hold values from -0.078125 to 0.078125
- key_weight_matrix: bfloat16 [5376, 2048], P(None, 'tp'), may hold values from -0.078125 to 0.078125
- value_weight_matrix: bfloat16 [5376, 2048], P(None, 'tp'), may hold values from -0.078125 to 0.078125
- query_gain: float32 [128], replicated, may hold values from 0.5 to 9
- key_norm_gain: float32 [128], replicated, may hold values from 0.5 to 9
- prior_key_cache: bfloat16 [1024, 2048], P(None, 'tp'), may hold values from -6 to 6
- prior_value_cache: bfloat16 [1024, 2048], P(None, 'tp'), may hold values from -6 to 6
- w_out: bfloat16 [4096, 5376], P('tp'), may hold values from -0.09375 to 0.09375
- post_gain: float32 [5376], replicated, may hold values from 0.5 to 2
Outputs:
- updated: bfloat16 [4096, 5376], P(('seq', 'tp'))
The draws below stay inside these ranges and needn't reach their ends.
All inputs are finite; a program needn't handle non-finite values.
Results may differ from the reference program's by a relative error of at most 0.015.
The reference program's roundings to bfloat16 on the way count: a program that leaves them out, or rounds other values in their place, can miss the bound.
Values may be sent and summed in bfloat16 or wider, within the bound.
A program may use at most 128 MiB of HBM per device.

```python
import math
import jax
import jax.numpy as jnp
from jax import lax

MODEL_WIDTH = 5376
HQ = 32
KEY_VALUE_HEADS = 16
HEAD_DIM = 128
WINDOW_SPAN = 1024
BLOCK_TOKENS = 4096
N_TP = 8


def gain_helper(key):
    low, high = (0.5, 2.0)
    logs = jax.random.uniform(key, (HEAD_DIM,), jnp.float32, math.log(low), math.log(high))
    return jnp.exp(logs).astype(jnp.float32)


def draw_query_gain(key, part):
    return gain_helper(jax.random.fold_in(key, 11))


def draw_key_norm_gain(key, part):
    return gain_helper(jax.random.fold_in(key, 12))


def block_scale(own_key, dims, shards, least, high):
    def one(axis_at, parts):
        steps = jax.random.uniform(jax.random.fold_in(jax.random.fold_in(own_key, 6), axis_at), (parts,), jnp.float32, least / len(shards), high / len(shards))
        return jnp.repeat(jnp.exp(steps), dims[axis_at] // parts).reshape((-1,) + (1,) * (len(dims) - axis_at - 1))

    level = one(*shards[0])
    for cut in shards[1:]:
        level = level * one(*cut)
    return level


def centred(own_key, dims, width, bound, shards=(), held_as=jnp.bfloat16):
    level = block_scale(own_key, dims, shards, -0.22, 0.18) if shards else 1.0
    entries = jax.random.normal(own_key, dims, jnp.float32) * width * level
    return jnp.minimum(jnp.maximum(entries, -bound), bound).astype(held_as)


def setup_inputs(seed: int = 0) -> dict:
    seeds = jax.random.split(jax.random.key(seed), 12)
    tokens = centred(seeds[0], (BLOCK_TOKENS, MODEL_WIDTH), 1.0, 6.0, ((0, 4),))
    pre_gain = jnp.clip(jnp.exp(jax.random.uniform(seeds[1], (MODEL_WIDTH,), jnp.float32, math.log(0.5), math.log(2.0))), 0.5, 2.0)
    w_query = centred(seeds[2], (MODEL_WIDTH, HQ * HEAD_DIM), MODEL_WIDTH ** -0.5, 0.078125, ((1, 8),))
    key_weight_matrix = centred(seeds[3], (MODEL_WIDTH, KEY_VALUE_HEADS * HEAD_DIM), MODEL_WIDTH ** -0.5, 0.078125, ((1, 8),))
    value_weight_matrix = centred(seeds[4], (MODEL_WIDTH, KEY_VALUE_HEADS * HEAD_DIM), MODEL_WIDTH ** -0.5, 0.078125, ((1, 8),))
    query_gain = draw_query_gain(jax.random.fold_in(seeds[11], 71), 0)
    key_norm_gain = draw_key_norm_gain(jax.random.fold_in(seeds[11], 71), 0)
    prior_key_cache = centred(seeds[7], (WINDOW_SPAN, KEY_VALUE_HEADS * HEAD_DIM), 1.0, 6.0, ((1, 8),))
    prior_value_cache = centred(seeds[8], (WINDOW_SPAN, KEY_VALUE_HEADS * HEAD_DIM), 1.0, 6.0, ((1, 8),))
    w_out = centred(seeds[9], (HQ * HEAD_DIM, MODEL_WIDTH), (HQ * HEAD_DIM) ** -0.5, 0.09375, ((0, 8),))
    post_gain = jnp.clip(jnp.exp(jax.random.uniform(seeds[10], (MODEL_WIDTH,), jnp.float32, math.log(0.5), math.log(2.0))), 0.5, 2.0)
    return dict(tokens=tokens, pre_gain=pre_gain, w_query=w_query, key_weight_matrix=key_weight_matrix, value_weight_matrix=value_weight_matrix, query_gain=query_gain, key_norm_gain=key_norm_gain, prior_key_cache=prior_key_cache, prior_value_cache=prior_value_cache, w_out=w_out, post_gain=post_gain)


EPSILON = 1e-06

def root_mean_norm(values, gain):
    mean_square = lax.optimization_barrier(jnp.mean(values * values, axis=-1, keepdims=True))
    return values * lax.rsqrt(mean_square + EPSILON) * gain

def rotary_embed_pairs(values, token_positions):
    half = values.shape[-1] // 2
    exponent = jnp.arange(half, dtype=jnp.float32) * (-2.0 / values.shape[-1])
    frequency = jnp.power(jnp.float32(10000.0), exponent)
    angles = token_positions.astype(jnp.float32)[:, None] * frequency[None, :]
    cosine = jnp.cos(angles)[:, None, :]
    sine = jnp.sin(angles)[:, None, :]
    first = values[..., :half]
    second = values[..., half:]
    return jnp.concatenate([first * cosine - second * sine, second * cosine + first * sine], axis=-1)

def attend_block(query_rows, key_rows, value_rows, scale):
    count = query_rows.shape[0]
    heads = query_rows.shape[1]
    kv_heads = key_rows.shape[1]
    grouped = query_rows.reshape(count, kv_heads, heads // kv_heads, -1).astype(jnp.float32)
    scores = jnp.einsum('bkgd,mkd->kgbm', grouped, key_rows.astype(jnp.float32)) * scale
    row_ids = lax.broadcasted_iota(jnp.int32, (count, key_rows.shape[0]), 0)
    col_ids = lax.broadcasted_iota(jnp.int32, (count, key_rows.shape[0]), 1)
    allowed = (col_ids > row_ids) & (col_ids <= row_ids + WINDOW_SPAN)
    scores = jnp.where(allowed, scores, -jnp.inf)
    highest = lax.optimization_barrier(jnp.max(scores, axis=-1, keepdims=True))
    weights = jnp.exp(scores - highest)
    weights = (weights / lax.optimization_barrier(jnp.sum(weights, axis=-1, keepdims=True))).astype(jnp.bfloat16)
    mixed = jnp.einsum('kgbm,mkd->bkgd', weights.astype(jnp.float32), value_rows.astype(jnp.float32))
    return mixed.astype(jnp.bfloat16).reshape(count, heads, -1)

def reference(tokens, pre_gain, w_query, key_weight_matrix, value_weight_matrix, query_gain, key_norm_gain, prior_key_cache, prior_value_cache, w_out, post_gain):
    inputs = tokens.astype(jnp.float32)
    normed = root_mean_norm(inputs, pre_gain).astype(jnp.bfloat16)
    query_raw = jnp.dot(normed, w_query, preferred_element_type=jnp.float32)
    unnormed_keys = jnp.dot(normed, key_weight_matrix, preferred_element_type=jnp.float32)
    projected_values = jnp.dot(normed, value_weight_matrix, preferred_element_type=jnp.float32)
    token_positions = WINDOW_SPAN + jnp.arange(BLOCK_TOKENS, dtype=jnp.int32)
    queries = rotary_embed_pairs(root_mean_norm(query_raw.reshape(BLOCK_TOKENS, HQ, HEAD_DIM), query_gain), token_positions).astype(jnp.bfloat16)
    block_keys = rotary_embed_pairs(root_mean_norm(unnormed_keys.reshape(BLOCK_TOKENS, KEY_VALUE_HEADS, HEAD_DIM), key_norm_gain), token_positions).astype(jnp.bfloat16)
    block_values = projected_values.astype(jnp.bfloat16).reshape(BLOCK_TOKENS, KEY_VALUE_HEADS, HEAD_DIM)
    joined_keys = jnp.concatenate([prior_key_cache.reshape(WINDOW_SPAN, KEY_VALUE_HEADS, HEAD_DIM), block_keys], axis=0)
    joined_values = jnp.concatenate([prior_value_cache.reshape(WINDOW_SPAN, KEY_VALUE_HEADS, HEAD_DIM), block_values], axis=0)
    size = min(512, BLOCK_TOKENS)
    scale = float(MODEL_WIDTH // HQ) ** (-0.5)

    def one_block(number):
        start = (number * size).astype(jnp.int32)
        query_rows = lax.dynamic_slice_in_dim(queries, start, size, 0)
        key_rows = lax.dynamic_slice_in_dim(joined_keys, start, size + WINDOW_SPAN, 0)
        value_rows = lax.dynamic_slice_in_dim(joined_values, start, size + WINDOW_SPAN, 0)
        return attend_block(query_rows, key_rows, value_rows, scale)
    blocks = lax.map(one_block, jnp.arange(BLOCK_TOKENS // size, dtype=jnp.int32))
    attended = blocks.reshape(BLOCK_TOKENS, HQ * HEAD_DIM)
    group_cols = HQ * HEAD_DIM // N_TP

    def add_group(total, group):
        begin = (group * group_cols).astype(jnp.int32)
        columns = lax.dynamic_slice_in_dim(attended, begin, group_cols, 1)
        rows = lax.dynamic_slice_in_dim(w_out, begin, group_cols, 0)
        term = jnp.dot(columns, rows, preferred_element_type=jnp.float32).astype(jnp.bfloat16)
        term = lax.optimization_barrier(term)
        return (total + term.astype(jnp.float32), None)
    summed, _ = lax.scan(add_group, jnp.zeros((BLOCK_TOKENS, MODEL_WIDTH), jnp.float32), jnp.arange(N_TP, dtype=jnp.int32))
    return (inputs + root_mean_norm(summed, post_gain)).astype(jnp.bfloat16)
```

```python
import functools

import jax
import jax.numpy as jnp
from jax import lax
from jax.experimental import pallas as pl
from jax.experimental.pallas import tpu as pltpu
from jax.sharding import PartitionSpec as P


MODEL_WIDTH = 5376
HQ = 32
WINDOW_SPAN = 1024


EPSILON = 1e-06


def shifted(value, axis, steps):
    count = lax.axis_size(axis)
    first, last = (max(0, -steps), min(count, count - steps))
    return lax.ppermute(value, axis, [(source, source + steps) for source in range(first, last)])


def swapped(value, axis, bit):
    count = lax.axis_size(axis)
    return lax.ppermute(value, axis, [(source, source ^ bit) for source in range(count)])


def turned(value, axis, steps):
    count = lax.axis_size(axis)
    return lax.ppermute(
        value, axis, [(source, (source + steps) % count) for source in range(count)]
    )


def root_mean_norm(values, gain):
    mean_square = jnp.mean(values * values, axis=-1, keepdims=True)
    return values * lax.rsqrt(mean_square + EPSILON) * gain


def rotary_tables(half, token_positions):
    exponent = jnp.arange(half, dtype=jnp.float32) * (-1.0 / half)
    frequency = jnp.power(jnp.float32(10000.0), exponent)
    angles = token_positions.astype(jnp.float32)[:, None] * frequency[None, :]
    return jnp.cos(angles), jnp.sin(angles)


def project_kernel(head_size, kinds, x_ref, w_ref, gain_ref, cos_ref, sin_ref, out_ref):
    raw = jnp.dot(x_ref[...], w_ref[...], preferred_element_type=jnp.float32)
    if not kinds:
        out_ref[...] = raw.astype(out_ref.dtype)
        return
    half = head_size // 2
    gain = gain_ref[...]
    cosine = cos_ref[...]
    sine = sin_ref[...]
    for head in range(raw.shape[1] // head_size):
        u = raw[:, head * head_size : (head + 1) * head_size]
        mean_square = jnp.mean(u * u, axis=-1, keepdims=True)
        u = u * lax.rsqrt(mean_square + EPSILON) * gain
        turned_u = pltpu.roll(u, half, 1)
        out_ref[:, head * head_size : (head + 1) * head_size] = (
            u * cosine + turned_u * sine
        ).astype(out_ref.dtype)


def project(normed, weight, gain, cosine, sine, rotate):
    rows, width = normed.shape
    cols = weight.shape[1]
    head_size = gain.shape[0]
    tile = min(256, cols)
    row_tile = min(512, rows)
    return pl.pallas_call(
        functools.partial(project_kernel, head_size, rotate),
        out_shape=jax.ShapeDtypeStruct((rows, cols), jnp.bfloat16),
        grid=(cols // tile, rows // row_tile),
        in_specs=[
            pl.BlockSpec((row_tile, width), lambda j, i: (i, 0)),
            pl.BlockSpec((width, tile), lambda j, i: (0, j)),
            pl.BlockSpec((1, head_size), lambda j, i: (0, 0)),
            pl.BlockSpec((row_tile, head_size), lambda j, i: (i, 0)),
            pl.BlockSpec((row_tile, head_size), lambda j, i: (i, 0)),
        ],
        out_specs=pl.BlockSpec((row_tile, tile), lambda j, i: (i, j)),
        compiler_params=pltpu.CompilerParams(vmem_limit_bytes=40 * 1024 * 1024),
        cost_estimate=pl.CostEstimate(
            flops=2 * rows * width * cols,
            bytes_accessed=2 * (rows * width + width * cols + rows * cols),
            transcendentals=0,
        ),
    )(normed, weight, gain[None, :], cosine, sine)


def attend_kernel(head_size, scale, start_ref, q_ref, k_ref, v_ref, out_ref):
    count = q_ref.shape[0]
    span = count + WINDOW_SPAN
    first = pl.multiple_of(start_ref[0] * count, count)
    keys = k_ref[pl.ds(first, span), :]
    values = v_ref[pl.ds(first, span), :]
    row_ids = lax.broadcasted_iota(jnp.int32, (count, span), 0)
    col_ids = lax.broadcasted_iota(jnp.int32, (count, span), 1)
    allowed = (col_ids > row_ids) & (col_ids <= row_ids + WINDOW_SPAN)
    for head in range(q_ref.shape[1] // head_size):
        cols = slice(head * head_size, (head + 1) * head_size)
        scores = lax.dot_general(
            q_ref[:, cols], keys, (((1,), (1,)), ((), ())), preferred_element_type=jnp.float32
        )
        scores = jnp.where(allowed, scores * scale, -jnp.inf)
        highest = jnp.max(scores, axis=-1, keepdims=True)
        weights = jnp.exp(scores - highest)
        total = jnp.sum(weights, axis=-1, keepdims=True)
        mixed = jnp.dot(weights.astype(jnp.bfloat16), values, preferred_element_type=jnp.float32)
        out_ref[:, cols] = (mixed / total).astype(out_ref.dtype)


def attend(start, queries, keys, values, head_size, count, scale):
    rows = keys.shape[0]
    kv_heads = keys.shape[1] // head_size
    group = queries.shape[1] // kv_heads
    span = count + WINDOW_SPAN
    heads = queries.shape[1] // head_size
    return pl.pallas_call(
        functools.partial(attend_kernel, head_size, scale),
        out_shape=jax.ShapeDtypeStruct((count, queries.shape[1]), jnp.bfloat16),
        grid_spec=pltpu.PrefetchScalarGridSpec(
            num_scalar_prefetch=1,
            grid=(kv_heads,),
            in_specs=[
                pl.BlockSpec((count, group), lambda h, s: (s[0], h)),
                pl.BlockSpec((rows, head_size), lambda h, s: (0, h)),
                pl.BlockSpec((rows, head_size), lambda h, s: (0, h)),
            ],
            out_specs=pl.BlockSpec((count, group), lambda h, s: (0, h)),
        ),
        compiler_params=pltpu.CompilerParams(vmem_limit_bytes=24 * 1024 * 1024),
        cost_estimate=pl.CostEstimate(
            flops=8 * heads * count * span * head_size,
            bytes_accessed=4 * rows * keys.shape[1],
            transcendentals=heads * count * span,
        ),
    )(jnp.full((1,), start, jnp.int32), queries, keys, values)


def partner_rows(w_out):
    seq = lax.axis_size("seq")
    seq_index = lax.axis_index("seq")
    rows = w_out.shape[0]
    share = rows // seq
    parts = 2
    piece = share // parts
    got = []
    for part in range(parts):
        mine = lax.dynamic_slice_in_dim(w_out, seq_index * share + part * piece, piece, 0)
        held = swapped(mine, "tp", 1)[None]
        bit = seq // 2
        while bit >= 1:
            other = swapped(held, "seq", bit)
            low = (seq_index & bit) == 0
            held = jnp.concatenate(
                [jnp.where(low, held, other), jnp.where(low, other, held)], axis=0
            )
            bit //= 2
        dims = []
        left = seq
        while left > 1:
            dims.append(2)
            left //= 2
        held = held.reshape(tuple(dims) + (piece, w_out.shape[1]))
        n = len(dims)
        held = held.transpose(tuple(reversed(range(n))) + (n, n + 1))
        got.append(held.reshape(seq, piece, w_out.shape[1]))
    return jnp.stack(got, axis=1).reshape(rows, w_out.shape[1])


def sublayer(
    tokens,
    pre_gain,
    w_query,
    key_weight_matrix,
    value_weight_matrix,
    query_gain,
    key_norm_gain,
    prior_key_cache,
    prior_value_cache,
    w_out,
    post_gain,
):
    seq_tokens = tokens.shape[0]
    tp = lax.axis_size("tp")
    local_rows = seq_tokens // tp
    head_size = query_gain.shape[0]
    seq_index = lax.axis_index("seq")
    tp_index = lax.axis_index("tp")
    side = tp_index % 2
    ring = tp // 2
    place = tp_index // 2
    count = 2 * local_rows

    w_other = partner_rows(w_out)

    normed = root_mean_norm(tokens.astype(jnp.float32), pre_gain).astype(jnp.bfloat16)
    token_positions = WINDOW_SPAN + seq_index * seq_tokens + jnp.arange(seq_tokens, dtype=jnp.int32)
    cosine, sine = rotary_tables(head_size // 2, token_positions)
    cosine = jnp.concatenate([cosine, cosine], axis=1)
    sine = jnp.concatenate([-sine, sine], axis=1)
    key_flat = project(normed, key_weight_matrix, key_norm_gain, cosine, sine, True)
    value_flat = project(normed, value_weight_matrix, key_norm_gain, cosine, sine, False)
    got_keys, got_values = shifted((key_flat, value_flat), "seq", 1)
    queries = project(normed, w_query, query_gain, cosine, sine, True)
    present = seq_index >= 1
    context_keys = jnp.concatenate(
        [jnp.where(present, got_keys, prior_key_cache), key_flat], axis=0
    )
    context_values = jnp.concatenate(
        [jnp.where(present, got_values, prior_value_cache), value_flat], axis=0
    )
    scale = float(MODEL_WIDTH // HQ) ** (-0.5)

    def halves(steps):
        block = (place + steps + ring) % ring
        mixed = attend(block, queries, context_keys, context_values, head_size, count, scale)
        own = lax.dynamic_slice_in_dim(mixed, side * local_rows, local_rows, 0)
        other = lax.dynamic_slice_in_dim(mixed, (1 - side) * local_rows, local_rows, 0)
        return own, other

    def products(distances):
        pairs = [halves(d) for d in distances]
        own = jnp.concatenate([p[0] for p in pairs], axis=0)
        got = swapped(jnp.concatenate([p[1] for p in pairs], axis=0), "tp", 1)
        return jnp.dot(own, w_out, preferred_element_type=jnp.float32) + jnp.dot(
            got, w_other, preferred_element_type=jnp.float32
        )

    middle = w_out.shape[1] // 2
    ahead = behind = None
    far = ring // 2
    if ring % 2 == 0:
        part = products([far]).astype(jnp.bfloat16)
        ahead = turned(part[:, :middle], "tp", 2)
        behind = turned(part[:, middle:], "tp", -2)
        far -= 1
    first = True
    for distance in range(far, 0, -1):
        part = products([distance, -distance])
        up, down = part[:local_rows], part[local_rows:]
        if ahead is not None:
            if first:
                up = jnp.concatenate([up[:, :middle] + ahead, up[:, middle:]], axis=1)
                down = jnp.concatenate([down[:, :middle], down[:, middle:] + behind], axis=1)
            else:
                up = up + ahead
                down = down + behind
        first = False
        ahead = turned(up.astype(jnp.bfloat16), "tp", 2)
        behind = turned(down.astype(jnp.bfloat16), "tp", -2)
    summed = products([0])
    if ahead is not None:
        if ahead.shape[1] != summed.shape[1]:
            summed = summed + jnp.concatenate([ahead, behind], axis=1).astype(jnp.float32)
        else:
            summed = summed + ahead.astype(jnp.float32) + behind.astype(jnp.float32)
    own_rows = lax.dynamic_slice_in_dim(tokens, tp_index * local_rows, local_rows, 0)
    return (own_rows.astype(jnp.float32) + root_mean_norm(summed, post_gain)).astype(jnp.bfloat16)


def solution(mesh):
    return jax.shard_map(
        sublayer,
        mesh=mesh,
        in_specs=(
            P("seq", None),
            P(),
            P(None, "tp"),
            P(None, "tp"),
            P(None, "tp"),
            P(),
            P(),
            P(None, "tp"),
            P(None, "tp"),
            P("tp", None),
            P(),
        ),
        out_specs=P(("seq", "tp"), None),
        check_vma=False,
    )
```
